256 devices in a mesh: row: 16 (over y_lo, x, core), col: 16 (over z, y_hi).
Axes of the slice: x: 4, y: 4 (y_hi: 2, y_lo: 2; y = y_hi * 2 + y_lo), z: 8, core: 2. Of those that a mesh axis runs over, the one named last changes fastest.
Arguments:
- collocation: bfloat16 [32768, 2048], P('col', 'row'), may hold values from -6 to 6
- greens: bfloat16 [2, 256, 2048], P(None, None, 'row'), may hold values from -0.0078125 to 0.0078125
- trial_orbitals: bfloat16 [256, 2048], P(None, 'row'), may hold values from -0.125 to 0.125
- coulomb: bfloat16 [16, 2048, 32768], P(None, 'row', 'col'), may hold values from -0.03125 to 0.03125
Outputs:
- gradient: bfloat16 [256, 2, 2048], P('col', None, 'row')
The draws below stay inside these ranges and needn't reach their ends.
All inputs are finite; a program needn't handle non-finite values.
Results may differ from the reference program's by a relative error of at most 0.039.
Values may be sent and summed in bfloat16 or wider, within the bound.
No kernel may reach another device: no remote copies, remote signals or barrier semaphores. Data moves between devices by JAX's collectives and lax.ppermute only.
A program may use at most 64 MiB of HBM per device.

```python
import jax
import jax.numpy as jnp
from jax import lax

P_SIZE = 32768
M = 2048
NOCC = 256
WALKERS = 2
N_ROW = 16
N_COL = 16


def shard_levels(rng, extent, pieces, least, high):
    def one(position, blocks):
        steps = jax.random.uniform(jax.random.fold_in(jax.random.fold_in(rng, 6), position), (blocks,), jnp.float32, least / len(pieces), high / len(pieces))
        return jnp.repeat(jnp.exp(steps), extent[position] // blocks).reshape((-1,) + (1,) * (len(extent) - position - 1))

    gain = one(*pieces[0])
    for cut in pieces[1:]:
        gain = gain * one(*cut)
    return gain


def noise(own_key, extent, spread, reach, split=(), kind=jnp.bfloat16):
    factor_of = shard_levels(own_key, extent, split, -0.22, 0.18) if split else 1.0
    entries = jax.random.normal(own_key, extent, jnp.float32) * spread * factor_of
    return jnp.minimum(jnp.maximum(entries, -reach), reach).astype(kind)


def setup_inputs(seed: int = 0) -> dict:
    splits = jax.random.split(jax.random.key(seed), 5)
    return {
        "collocation": noise(splits[0], (P_SIZE, M), 1.0, 6.0, ((0, 16), (1, 16))),
        "greens": noise(splits[1], (WALKERS, NOCC, M), (M * NOCC) ** -0.5, 0.0078125, ((2, 16),)),
        "trial_orbitals": noise(splits[2], (NOCC, M), M ** -0.5, 0.125, ((1, 16),)),
        "coulomb": noise(splits[3], (N_COL, P_SIZE // N_COL, P_SIZE), P_SIZE ** -0.5, 0.03125, ((1, 16), (2, 16))),
    }


def reference(collocation, greens, trial_orbitals, coulomb):
    stacked = jnp.concatenate([trial_orbitals[None], greens], axis=0).reshape((WALKERS + 1) * NOCC, M)
    shard_width = M // N_ROW
    encoded_sum = jnp.zeros((P_SIZE, (WALKERS + 1) * NOCC), jnp.float32)
    for group in range(N_ROW):
        left = collocation[:, group * shard_width:(group + 1) * shard_width].astype(jnp.float32)
        right = stacked[:, group * shard_width:(group + 1) * shard_width].astype(jnp.float32)
        partial_value = jnp.dot(left, right.T, precision=lax.Precision.HIGHEST)
        rounded = lax.optimization_barrier(partial_value.astype(jnp.bfloat16))
        encoded_sum = encoded_sum + rounded.astype(jnp.float32)
    encoded = encoded_sum.astype(jnp.bfloat16)
    orbit = encoded[:, :NOCC]
    orbit_wide = orbit.astype(jnp.float32)
    kernel = coulomb.reshape(P_SIZE, P_SIZE)
    height = min(1024, P_SIZE)
    kernel_blocks = kernel.reshape(P_SIZE // height, height, P_SIZE)
    orbit_blocks = orbit.reshape(P_SIZE // height, height, NOCC)
    results = []
    for walker in range(WALKERS):
        theta = encoded[:, (walker + 1) * NOCC:(walker + 2) * NOCC]
        theta_blocks = theta.reshape(P_SIZE // height, height, NOCC)

        def advance(totals, inputs):
            exchange_sum, potential = totals
            x_block, theta_block, v_block = inputs
            x_wide = x_block.astype(jnp.float32)
            theta_wide = theta_block.astype(jnp.float32)
            v_wide = v_block.astype(jnp.float32)
            t_tile = jnp.dot(theta_wide, orbit_wide.T, precision=lax.Precision.HIGHEST)
            amplitude = (v_wide * t_tile).astype(jnp.bfloat16).astype(jnp.float32)
            exchange_sum = exchange_sum + jnp.dot(amplitude.T, x_wide, precision=lax.Precision.HIGHEST)
            density = jnp.sum(x_wide * theta_wide, axis=1).astype(jnp.bfloat16).astype(jnp.float32)
            potential = potential + jnp.dot(density, v_wide, precision=lax.Precision.HIGHEST)
            return (exchange_sum, potential), None

        start_totals = (jnp.zeros((P_SIZE, NOCC), jnp.float32), jnp.zeros((P_SIZE,), jnp.float32))
        (exchange_sum, potential), unused = lax.scan(advance, start_totals, (orbit_blocks, theta_blocks, kernel_blocks))
        force_walker = (potential[:, None] * orbit_wide - exchange_sum).astype(jnp.bfloat16)
        decoded = jnp.dot(force_walker.astype(jnp.float32).T, collocation.astype(jnp.float32), precision=lax.Precision.HIGHEST)
        results.append(decoded * (P_SIZE ** -0.5))
    return jnp.stack(results, axis=1).astype(jnp.bfloat16)
```

```python
import jax
import jax.numpy as jnp
from jax import lax
from jax.experimental import pallas as pl
from jax.experimental.pallas import tpu as pltpu
from jax.sharding import Mesh
from jax.sharding import PartitionSpec as P

P_SIZE = 32768
ROW = ("yl", "x", "c")
CHIPS = ("yl", "x")
COL = ("z", "yh")
F32 = jnp.float32
BF16 = jnp.bfloat16
PAY = 784
LIMIT = pltpu.CompilerParams(vmem_limit_bytes=24 * 1024 * 1024)
VM = pl.BlockSpec(memory_space=pltpu.VMEM)
SM = pl.BlockSpec(memory_space=pltpu.SMEM)
HB = pl.BlockSpec(memory_space=pltpu.HBM)


def swap():
    return [(0, 1), (1, 0)]


def ring(size, step):
    return [(i, (i + step) % size) for i in range(size)]


def dot(a, b, dims):
    return lax.dot_general(a, b, (dims, ((), ())), preferred_element_type=F32)


def cost(flops, moved):
    return pl.CostEstimate(flops=flops, transcendentals=0, bytes_accessed=moved)


def encode_kernel(mine, got, trial, greens, other, out):
    def step(j, _):
        rows = jnp.concatenate([mine[j], got[j]], axis=1)
        x_side = jnp.concatenate([trial[...], other[0:256]], axis=1)
        out[j, 0:256] = dot(x_side, rows, ((1,), (1,))).astype(BF16)
        for w in range(2):
            side = jnp.concatenate([greens[w], other[256 * (w + 1):256 * (w + 2)]], axis=1)
            theta = dot(rows, side, ((1,), (1,))).astype(BF16)
            for h in range(2):
                at = 256 * (w + 1) + 128 * h
                out[j, at:at + 128] = theta[:, 128 * h:128 * (h + 1)]
        return 0

    lax.fori_loop(0, 8, step, 0, unroll=2)


def encode(*args):
    return pl.pallas_call(
        encode_kernel,
        in_specs=[VM] * 5,
        out_specs=VM,
        out_shape=jax.ShapeDtypeStruct((8, 768, 128), BF16),
        compiler_params=LIMIT,
        cost_estimate=cost(2 * 1024 * 256 * 768, 3 << 20),
        name="encode",
    )(*args)


def own_kernel(parts, out, spread):
    total = parts[0].astype(F32)
    for j in range(1, 8):
        total = total + parts[j].astype(F32)
    total = total.astype(BF16)
    out[0:768] = total
    for j in range(8):
        spread[j] = total[0:256]
    wide = total.astype(F32)
    rows = []
    for w in range(2):
        at = 256 * (w + 1)
        acc = jnp.sum(wide[0:128] * wide[at:at + 128].T, axis=0, keepdims=True)
        acc = acc + jnp.sum(wide[128:256] * wide[at + 128:at + 256].T, axis=0, keepdims=True)
        rows.append(acc)
    rows.append(jnp.zeros((14, 128), F32))
    out[768:784] = jnp.concatenate(rows, axis=0).astype(BF16)


def own_points(parts):
    return pl.pallas_call(
        own_kernel,
        in_specs=[VM],
        out_specs=[VM, VM],
        out_shape=[jax.ShapeDtypeStruct((PAY, 128), BF16), jax.ShapeDtypeStruct((8, 256, 128), BF16)],
        compiler_params=LIMIT,
        cost_estimate=cost(1 << 24, 2 << 20),
        name="own",
    )(parts)


def make_exchange_kernel(blocks, where, first, last):
    def kernel(pos, *refs):
        pays = refs[:blocks]
        kern, same, cross = refs[blocks:blocks + 3]
        rest = refs[blocks + 3:]
        v_buf, sems = rest[-2:]
        rest = rest[:-2]
        if not first:
            e_in, u_in = rest[:2]
            rest = rest[2:]
        core = pos[0]
        copies = []
        for h in range(2):
            for b in range(blocks):
                lanes = pl.ds(1024 * h, 1024)
                copies.append(
                    pltpu.make_async_copy(
                        kern.at[pos[1 + where[b]], :, lanes],
                        v_buf.at[h, pl.ds(128 * b, 128)],
                        sems.at[h, b],
                    )
                )
        for cp in copies:
            cp.start()
        xp = jnp.concatenate([p[0:256] for p in pays], axis=1)
        dens = jnp.concatenate([p[768:784] for p in pays], axis=1)

        def theta(w):
            at = 256 * (w + 1)
            return jnp.concatenate(
                [jnp.concatenate([p[at:at + 128], p[at + 128:at + 256]], axis=1) for p in pays], axis=0
            )

        flag = core == 0
        for h in range(2):
            for b in range(blocks):
                copies[h * blocks + b].wait()

            def chip_step(i, _):
                chip = 4 * h + i
                lanes = pl.ds(pl.multiple_of(256 * chip, 256), 256)
                a = same[chip]
                b = cross[chip]
                xq = jnp.concatenate([jnp.where(flag, a, b), jnp.where(flag, b, a)], axis=1)
                v = v_buf[h, :, pl.ds(pl.multiple_of(256 * i, 256), 256)]
                u = dot(dens, v, ((1,), (0,)))
                if not first:
                    u = u + u_in[:, lanes]
                if not last:
                    rest[1][:, lanes] = u
                wide = v.astype(F32)
                for w in range(2):
                    tile = dot(theta(w), xq, ((1,), (0,)))
                    amp = (wide * tile).astype(BF16)
                    e = dot(xp, amp, ((1,), (0,)))
                    rows = slice(256 * w, 256 * (w + 1))
                    if not first:
                        e = e + e_in[rows, lanes]
                    if not last:
                        rest[0][rows, lanes] = e
                    else:
                        f = (u[w:w + 1] * xq.astype(F32) - e).astype(BF16)
                        here = pl.ds(pl.multiple_of(128 * chip, 128), 128)
                        low, high = f[:, 0:128], f[:, 128:256]
                        rest[0][rows, here] = jnp.where(flag, low, high)
                        rest[1][rows, here] = jnp.where(flag, high, low)
                return 0

            lax.fori_loop(0, 4, chip_step, 0)

    return kernel


def exchange(pos, pays, where, coulomb, same, cross, totals, last):
    blocks = len(pays)
    first = totals is None
    args = [pos, *pays, coulomb, same, cross]
    in_specs = [SM] + [VM] * blocks + [HB, VM, VM]
    alias = {}
    if not first:
        if not last:
            alias = {len(args): 0, len(args) + 1: 1}
        args += list(totals)
        in_specs += [VM, VM]
    if last:
        out_shape = [jax.ShapeDtypeStruct((512, 1024), BF16)] * 2
    else:
        out_shape = [jax.ShapeDtypeStruct((512, 2048), F32), jax.ShapeDtypeStruct((16, 2048), F32)]
    rows = 128 * blocks
    return pl.pallas_call(
        make_exchange_kernel(blocks, where, first, last),
        in_specs=in_specs,
        out_specs=[VM, VM],
        out_shape=out_shape,
        scratch_shapes=[pltpu.VMEM((2, rows, 1024), BF16), pltpu.SemaphoreType.DMA((2, blocks))],
        input_output_aliases=alias,
        compiler_params=LIMIT,
        cost_estimate=cost(8 * rows * 2048 * 256, 8 << 20),
        name="exchange",
    )(*args)


def decode_kernel(pos, f_mine, f_got, *refs):
    cols = refs[:8]
    keep, give = refs[8:]
    f = (f_mine[...].astype(F32) + f_got[...].astype(F32)).astype(BF16)
    for j in range(8):
        chip = lax.bitwise_xor(pos[17], j // 4) * 4 + lax.rem(pos[18] - j % 4 + 4, 4)
        g = dot(f, jnp.concatenate([cols[j][0], cols[j][1]], axis=1), ((1,), (0,)))
        keep[chip] = g[:, 0:128].astype(BF16)
        give[chip] = g[:, 128:256].astype(BF16)


def decode(pos, f, f_got, cols):
    return pl.pallas_call(
        decode_kernel,
        in_specs=[SM] + [VM] * 10,
        out_specs=[VM, VM],
        out_shape=[jax.ShapeDtypeStruct((8, 512, 128), BF16)] * 2,
        compiler_params=LIMIT,
        cost_estimate=cost(2 * 512 * 1024 * 2048, 8 << 20),
        name="decode",
    )(pos, f, f_got, *cols)


def sum_kernel(parts, out):
    total = parts[0].astype(F32)
    for j in range(1, 8):
        total = total + parts[j].astype(F32)
    total = total.astype(BF16)
    for w in range(2):
        for c in range(16):
            out[c, w] = total[256 * w + 16 * c:256 * w + 16 * (c + 1)]


def x_shift(a, step):
    return lax.ppermute(a, "x", ring(4, step))


def on_device(collocation, greens, trial_orbitals, coulomb):
    yl, x, c = lax.axis_index("yl"), lax.axis_index("x"), lax.axis_index("c")
    z, yh = lax.axis_index("z"), lax.axis_index("yh")
    near = [(0, 0)] + [(s, 0) for s in (1, 2, 3, 4)] + [(-s, 0) for s in (1, 2, 3)]
    near += [(0, 1)] + [(s, 1) for s in (1, 2, 3)] + [(-s, 1) for s in (1, 2, 3, 4)]
    index = {key: n for n, key in enumerate(near)}
    places = [lax.rem(z - s + 8, 8) * 2 + (yh if flip == 0 else 1 - yh) for s, flip in near]
    pos = jnp.stack([c, *places, yl, x]).astype(jnp.int32)

    halves = collocation.reshape(8, 2, 128, 128)
    mine = lax.dynamic_index_in_dim(halves, c, 1, keepdims=False)
    give = lax.dynamic_index_in_dim(halves, 1 - c, 1, keepdims=False)
    stacked = jnp.concatenate([trial_orbitals, greens.reshape(512, 128)], axis=0)
    got = lax.ppermute(give, "c", swap())
    other = lax.ppermute(stacked, "c", swap())
    partial_value = encode(mine, got, trial_orbitals, greens, other)
    parts = lax.all_to_all(partial_value, CHIPS, 0, 0, tiled=True)
    own, spread = own_points(parts)

    pay = {(0, 0): own}
    pay[(0, 1)] = lax.ppermute(own, "yh", swap())

    def hop(s):
        for flip in (0, 1):
            for sign in (1, -1):
                if (sign * s, flip) in index:
                    pay[(sign * s, flip)] = lax.ppermute(
                        pay[(sign * (s - 1), flip)], "z", ring(8, sign)
                    )

    hop(1)
    same = lax.all_to_all(spread, CHIPS, 0, 0, tiled=True)
    cross = lax.ppermute(same, "c", swap())

    def held(keys, others):
        got = lax.optimization_barrier(tuple(pay[k] for k in keys) + tuple(others))
        for k, v in zip(keys, got):
            pay[k] = v
        return got[len(keys):]

    def stage(s):
        return [k for k in near if abs(k[0]) == s]

    def add(stages, totals, last=False):
        keys = [k for k in near if abs(k[0]) in stages]
        return exchange(pos, [pay[k] for k in keys], [index[k] for k in keys], coulomb, same, cross, totals, last)

    base = jnp.stack([mine.reshape(1024, 128), got.reshape(1024, 128)])
    base, same = lax.optimization_barrier((base, same))
    cols = [base] + [None] * 7
    cols[4] = lax.ppermute(base, "yl", swap())
    cols[1] = x_shift(base, 1)
    cols[3] = x_shift(base, -1)
    hop(2)
    totals = add((0, 1), None)
    cols[4], cols[1], cols[3] = held(stage(2), (cols[4], cols[1], cols[3]))
    cols[5] = x_shift(cols[4], 1)
    cols[7] = x_shift(cols[4], -1)
    cols[2] = x_shift(cols[1], 1)
    hop(3)
    totals = add((2,), totals)
    cols[2], cols[5], cols[7] = held(stage(3), (cols[2], cols[5], cols[7]))
    cols[6] = lax.ppermute(cols[2], "yl", swap())
    hop(4)
    totals = add((3,), totals)
    f_mine, f_give = add((4,), totals, True)
    f_got = lax.ppermute(f_give, "c", swap())
    keep, send = decode(pos, f_mine, f_got, cols)
    back = lax.ppermute(send, "c", swap())
    both = (keep.astype(F32) + back.astype(F32)).astype(BF16)
    terms = lax.all_to_all(both, CHIPS, 0, 0, tiled=True)
    summed = pl.pallas_call(
        sum_kernel,
        in_specs=[VM],
        out_specs=VM,
        out_shape=jax.ShapeDtypeStruct((16, 2, 16, 128), BF16),
        compiler_params=LIMIT,
        name="chip_sum",
    )(terms)
    shares = lax.all_to_all(summed, COL, 0, 0, tiled=True)
    total = jnp.sum(shares.astype(F32), axis=0) * P_SIZE ** (-0.5)
    return jnp.swapaxes(total, 0, 1).astype(BF16)


def solution(mesh):
    finer = Mesh(mesh.devices.reshape(2, 4, 2, 8, 2), ("yl", "x", "c", "z", "yh"))
    placed = (P(COL, ROW), P(None, None, ROW), P(None, ROW), P(None, ROW, COL))
    return jax.shard_map(
        on_device, mesh=finer, in_specs=placed, out_specs=P(COL, None, ROW), check_vma=False
    )
```

```python
import jax
import jax.numpy as jnp
from jax import lax
from jax.experimental import pallas as pl
from jax.experimental.pallas import tpu as pltpu
from jax.sharding import Mesh
from jax.sharding import PartitionSpec as P

P_SIZE = 32768
ROW = ("yl", "x", "c")
CHIPS = ("yl", "x")
COL = ("z", "yh")
F32 = jnp.float32
BF16 = jnp.bfloat16
PAY = 784
LIMIT = pltpu.CompilerParams(vmem_limit_bytes=16 * 1024 * 1024)
VM = pl.BlockSpec(memory_space=pltpu.VMEM)
SM = pl.BlockSpec(memory_space=pltpu.SMEM)
HB = pl.BlockSpec(memory_space=pltpu.HBM)


def swap():
    return [(0, 1), (1, 0)]


def ring(size, step):
    return [(i, (i + step) % size) for i in range(size)]


def dot(a, b, dims):
    return lax.dot_general(a, b, (dims, ((), ())), preferred_element_type=F32)


def cost(flops, moved):
    return pl.CostEstimate(flops=flops, transcendentals=0, bytes_accessed=moved)


def encode_kernel(mine, got, stacked, other, out):
    def step(j, _):
        rows = jnp.concatenate([mine[j], got[j]], axis=1)
        x_side = jnp.concatenate([stacked[0:256], other[0:256]], axis=1)
        out[j, :, 0:128] = dot(x_side, rows, ((1,), (1,))).astype(BF16)
        for w in range(2):
            here = slice(256 * (w + 1), 256 * (w + 2))
            side = jnp.concatenate([stacked[here], other[here]], axis=1)
            theta = dot(rows, side, ((1,), (1,))).astype(BF16)
            for h in range(2):
                lanes = slice(128 * (w + 1), 128 * (w + 2))
                out[j, 128 * h:128 * (h + 1), lanes] = theta[:, 128 * h:128 * (h + 1)]
        return 0

    lax.fori_loop(0, 8, step, 0, unroll=2)


def encode(*args):
    return pl.pallas_call(
        encode_kernel,
        in_specs=[VM] * 4,
        out_specs=VM,
        out_shape=jax.ShapeDtypeStruct((8, 256, 384), BF16),
        compiler_params=LIMIT,
        cost_estimate=cost(2 * 1024 * 256 * 768, 3 << 20),
        name="encode",
    )(*args)


def own_kernel(parts, out, spread):
    total = parts[0].astype(F32)
    for j in range(1, 8):
        total = total + parts[j].astype(F32)
    total = jnp.concatenate([total[:, 128 * n:128 * (n + 1)] for n in range(3)], axis=0).astype(BF16)
    out[0:768] = total
    for j in range(8):
        spread[j] = total[0:256]
    wide = total.astype(F32)
    rows = []
    for w in range(2):
        at = 256 * (w + 1)
        acc = jnp.sum(wide[0:128] * wide[at:at + 128].T, axis=0, keepdims=True)
        acc = acc + jnp.sum(wide[128:256] * wide[at + 128:at + 256].T, axis=0, keepdims=True)
        rows.append(acc)
    rows.append(jnp.zeros((14, 128), F32))
    out[768:784] = jnp.concatenate(rows, axis=0).astype(BF16)


def own_points(parts):
    return pl.pallas_call(
        own_kernel,
        in_specs=[VM],
        out_specs=[VM, VM],
        out_shape=[jax.ShapeDtypeStruct((PAY, 128), BF16), jax.ShapeDtypeStruct((8, 256, 128), BF16)],
        compiler_params=LIMIT,
        cost_estimate=cost(1 << 24, 2 << 20),
        name="own",
    )(parts)


def make_exchange_kernel(shapes, where, first, last):
    def kernel(pos, *refs):
        held = refs[:len(shapes)]
        pays = []
        for ref, shape in zip(held, shapes):
            pays += [ref] if len(shape) == 2 else [ref.at[0], ref.at[1]]
        kern, same, cross = refs[len(shapes):len(shapes) + 3]
        rest = refs[len(shapes) + 3:]
        if not first:
            e_in, u_in = rest[:2]
            rest = rest[2:]
        v_buf, sems = rest[-2:]
        rest = rest[:-2]
        flag = pos[0] == 0

        def fetch(h, b):
            lanes = pl.ds(pl.multiple_of(512 * h, 512), 512)
            return pltpu.make_async_copy(
                kern.at[pos[1 + where[b]], :, lanes], v_buf.at[h, pl.ds(128 * b, 128)], sems.at[h, b]
            )

        for h in range(4):
            for b in range(len(where)):
                fetch(h, b).start()

        def theta(w):
            at = 256 * (w + 1)
            return jnp.concatenate(
                [jnp.concatenate([p[at:at + 128], p[at + 128:at + 256]], axis=1) for p in pays], axis=0
            )

        def pair_step(h, _):
            for b in range(len(where)):
                fetch(h, b).wait()
            for half in range(2):
                chip_step(h, half)
            return 0

        def chip_step(h, half):
            chip = 2 * h + half
            xp = jnp.concatenate([p[0:256] for p in pays], axis=1)
            dens = jnp.concatenate([p[768:784] for p in pays], axis=1)
            lanes = pl.ds(pl.multiple_of(256 * chip, 256), 256)
            a = same[chip]
            b = cross[chip]
            xq = jnp.concatenate([jnp.where(flag, a, b), jnp.where(flag, b, a)], axis=1)
            v = v_buf[h, :, 256 * half:256 * (half + 1)]
            u = dot(dens, v, ((1,), (0,)))
            if not first:
                u = u + u_in[:, lanes]
            if not last:
                rest[1][:, lanes] = u
            wide = v.astype(F32)
            for w in range(2):
                tile = dot(theta(w), xq, ((1,), (0,)))
                amp = (wide * tile).astype(BF16)
                e = dot(xp, amp, ((1,), (0,)))
                rows = slice(256 * w, 256 * (w + 1))
                if not first:
                    e = e + e_in[rows, lanes]
                if not last:
                    rest[0][rows, lanes] = e
                else:
                    f = (u[w:w + 1] * xq.astype(F32) - e).astype(BF16)
                    here = pl.ds(pl.multiple_of(128 * chip, 128), 128)
                    low, high = f[:, 0:128], f[:, 128:256]
                    rest[0][rows, here] = jnp.where(flag, low, high)
                    rest[1][rows, here] = jnp.where(flag, high, low)

        lax.fori_loop(0, 4, pair_step, 0)

    return kernel


def exchange(pos, held, where, coulomb, same, cross, totals, last):
    first = totals is None
    args = [pos, *held, coulomb, same, cross]
    in_specs = [SM] + [VM] * len(held) + [HB, VM, VM]
    alias = {}
    if not first:
        if not last:
            alias = {len(args): 0, len(args) + 1: 1}
        args += list(totals)
        in_specs += [VM, VM]
    if last:
        out_shape = [jax.ShapeDtypeStruct((512, 1024), BF16)] * 2
    else:
        out_shape = [jax.ShapeDtypeStruct((512, 2048), F32), jax.ShapeDtypeStruct((16, 2048), F32)]
    rows = 128 * len(where)
    return pl.pallas_call(
        make_exchange_kernel([a.shape for a in held], where, first, last),
        in_specs=in_specs,
        out_specs=[VM, VM],
        out_shape=out_shape,
        scratch_shapes=[pltpu.VMEM((4, rows, 512), BF16), pltpu.SemaphoreType.DMA((4, len(where)))],
        input_output_aliases=alias,
        compiler_params=LIMIT,
        cost_estimate=cost(8 * rows * 2048 * 256, 8 << 20),
        name="exchange",
    )(*args)


def decode_kernel(pos, f_mine, f_got, *refs):
    cols = refs[:8]
    keep, give = refs[8:]
    f = (f_mine[...].astype(F32) + f_got[...].astype(F32)).astype(BF16)
    for j in range(8):
        chip = lax.bitwise_xor(pos[17], j // 4) * 4 + lax.rem(pos[18] - j % 4 + 4, 4)
        g = dot(f, jnp.concatenate([cols[j][0], cols[j][1]], axis=1), ((1,), (0,)))
        keep[chip] = g[:, 0:128].astype(BF16)
        give[chip] = g[:, 128:256].astype(BF16)


def decode(pos, f, f_got, cols):
    return pl.pallas_call(
        decode_kernel,
        in_specs=[SM] + [VM] * 10,
        out_specs=[VM, VM],
        out_shape=[jax.ShapeDtypeStruct((8, 512, 128), BF16)] * 2,
        compiler_params=LIMIT,
        cost_estimate=cost(2 * 512 * 1024 * 2048, 8 << 20),
        name="decode",
    )(pos, f, f_got, *cols)


def sum_kernel(parts, out):
    total = parts[0].astype(F32)
    for j in range(1, 8):
        total = total + parts[j].astype(F32)
    total = total.astype(BF16)
    for w in range(2):
        for c in range(16):
            out[c, w] = total[256 * w + 16 * c:256 * w + 16 * (c + 1)]


def program(collocation, greens, trial_orbitals, coulomb):
    yl, x, c = lax.axis_index("yl"), lax.axis_index("x"), lax.axis_index("c")
    z, yh = lax.axis_index("z"), lax.axis_index("yh")

    def place(step, flip):
        return lax.rem(z - step + 8, 8) * 2 + (yh if flip == 0 else 1 - yh)

    order = [(0, 0), (0, 1)]
    for s in (1, 2, 3):
        order += [(s, 0), (s, 1), (-s, 0), (-s, 1)]
    order += [(4, 0), (-4, 1)]
    pos = jnp.stack([c] + [place(*k) for k in order] + [yl, x]).astype(jnp.int32)

    coulomb = pltpu.with_memory_space_constraint(coulomb, pltpu.HBM)
    halves = collocation.reshape(8, 2, 128, 128)
    mine = lax.dynamic_index_in_dim(halves, c, 1, keepdims=False)
    give = lax.dynamic_index_in_dim(halves, 1 - c, 1, keepdims=False)
    stacked = jnp.concatenate([trial_orbitals, greens.reshape(512, 128)], axis=0)
    got = lax.ppermute(give, "c", swap())
    other = lax.ppermute(stacked, "c", swap())
    partial_value = encode(mine, got, stacked, other)
    parts = lax.all_to_all(partial_value, CHIPS, 0, 0, tiled=True)
    own, spread = own_points(parts)

    mate = lax.ppermute(own, "yh", swap())
    pair = jnp.stack([own, mate])
    same = lax.all_to_all(spread, CHIPS, 0, 0, tiled=True)
    cross = lax.ppermute(same, "c", swap())
    up, down = [pair], [pair]
    for _ in range(3):
        up.append(lax.ppermute(up[-1], "z", ring(8, 1)))
        down.append(lax.ppermute(down[-1], "z", ring(8, -1)))
    last_up, last_down = up[3][0], down[3][1]
    far_up = lax.ppermute(last_up, "z", ring(8, 1))
    far_down = lax.ppermute(last_down, "z", ring(8, -1))
    far = [far_up, far_down]
    base = jnp.stack([mine.reshape(1024, 128), got.reshape(1024, 128)])
    base, _ = lax.optimization_barrier((base, pair))
    cols = [base] + [None] * 7
    cols[4] = lax.ppermute(base, "yl", swap())
    cols[1] = lax.ppermute(base, "x", ring(4, 1))
    cols[3] = lax.ppermute(base, "x", ring(4, -1))
    cols[2] = lax.ppermute(cols[1], "x", ring(4, 1))
    cols[7] = lax.ppermute(cols[4], "x", ring(4, -1))
    cols[5] = lax.ppermute(cols[4], "x", ring(4, 1))
    cols[6] = lax.ppermute(cols[2], "yl", swap())
    totals = exchange(pos, [pair, up[1], down[1]], list(range(6)), coulomb, same, cross, None, False)
    totals = exchange(pos, [up[2], down[2]], [6, 7, 8, 9], coulomb, same, cross, totals, False)
    f_mine, f_give = exchange(pos, [up[3], down[3], *far], [10, 11, 12, 13, 14, 15], coulomb, same, cross, totals, True)
    f_got = lax.ppermute(f_give, "c", swap())
    keep, send = decode(pos, f_mine, f_got, cols)
    back = lax.ppermute(send, "c", swap())
    both = (keep.astype(F32) + back.astype(F32)).astype(BF16)
    terms = lax.all_to_all(both, CHIPS, 0, 0, tiled=True)
    summed = pl.pallas_call(
        sum_kernel,
        in_specs=[VM],
        out_specs=VM,
        out_shape=jax.ShapeDtypeStruct((16, 2, 16, 128), BF16),
        compiler_params=LIMIT,
        name="chip_sum",
    )(terms)
    shares = lax.all_to_all(summed.reshape(16, 32, 128), COL, 0, 0, tiled=True).reshape(16, 2, 16, 128)
    total = jnp.sum(shares.astype(F32), axis=0) * P_SIZE ** (-0.5)
    return jnp.swapaxes(total, 0, 1).astype(BF16)


def solution(mesh):
    finer = Mesh(mesh.devices.reshape(2, 4, 2, 8, 2), ("yl", "x", "c", "z", "yh"))
    placed = (P(COL, ROW), P(None, None, ROW), P(None, ROW), P(None, ROW, COL))
    return jax.shard_map(program, mesh=finer, in_specs=placed, out_specs=P(COL, None, ROW), check_vma=False)
```

```python
import jax
import jax.numpy as jnp
from jax import lax
from jax.experimental import pallas as pl
from jax.experimental.pallas import tpu as pltpu
from jax.sharding import Mesh
from jax.sharding import PartitionSpec as P

P_SIZE = 32768
ROW = ("yl", "x", "c")
CHIPS = ("yl", "x")
COL = ("z", "yh")
F32 = jnp.float32
BF16 = jnp.bfloat16
PAY = 784
NEAR, MIDDLE, LAST = range(0, 6), range(6, 10), range(10, 16)
LIMIT = pltpu.CompilerParams(vmem_limit_bytes=8 * 1024 * 1024)
VM = pl.BlockSpec(memory_space=pltpu.VMEM)
SM = pl.BlockSpec(memory_space=pltpu.SMEM)
HB = pl.BlockSpec(memory_space=pltpu.HBM)


def swap():
    return [(0, 1), (1, 0)]


def ring(size, step):
    return [(i, (i + step) % size) for i in range(size)]


def dot(a, b, dims):
    return lax.dot_general(a, b, (dims, ((), ())), preferred_element_type=F32)


def cost(flops, moved):
    return pl.CostEstimate(flops=flops, transcendentals=0, bytes_accessed=moved)


def encode_kernel(mine, got, stacked, other, out):
    def step(j, _):
        rows = jnp.concatenate([mine[j], got[j]], axis=1)
        x_side = jnp.concatenate([stacked[0:256], other[0:256]], axis=1)
        out[j, :, 0:128] = dot(x_side, rows, ((1,), (1,))).astype(BF16)
        for w in range(2):
            here = slice(256 * (w + 1), 256 * (w + 2))
            side = jnp.concatenate([stacked[here], other[here]], axis=1)
            theta = dot(rows, side, ((1,), (1,))).astype(BF16)
            for h in range(2):
                lanes = slice(128 * (w + 1), 128 * (w + 2))
                out[j, 128 * h:128 * (h + 1), lanes] = theta[:, 128 * h:128 * (h + 1)]
        return 0

    lax.fori_loop(0, 8, step, 0, unroll=2)


def encode(*args):
    return pl.pallas_call(
        encode_kernel,
        in_specs=[VM] * 4,
        out_specs=VM,
        out_shape=jax.ShapeDtypeStruct((8, 256, 384), BF16),
        compiler_params=LIMIT,
        cost_estimate=cost(2 * 1024 * 256 * 768, 3 << 20),
        name="encode",
    )(*args)


def fetch_kernel(pos, kern, rows, sems):
    copies = [pltpu.make_async_copy(kern.at[pos[1 + n]], rows.at[n], sems.at[n]) for n in range(16)]
    for copy in copies:
        copy.start()
    for copy in copies:
        copy.wait()


def fetch(pos, coulomb):
    return pl.pallas_call(
        fetch_kernel,
        in_specs=[SM, HB],
        out_specs=VM,
        out_shape=jax.ShapeDtypeStruct((16, 128, 2048), BF16),
        scratch_shapes=[pltpu.SemaphoreType.DMA((16,))],
        compiler_params=LIMIT,
        cost_estimate=cost(1 << 20, 8 << 20),
        name="fetch",
    )(pos, coulomb)


def own_kernel(parts, out, spread):
    total = parts[0].astype(F32)
    for j in range(1, 8):
        total = total + parts[j].astype(F32)
    total = jnp.concatenate([total[:, 128 * n:128 * (n + 1)] for n in range(3)], axis=0).astype(BF16)
    out[0:768] = total
    for j in range(8):
        spread[j] = total[0:256]
    wide = total.astype(F32)
    sums = []
    for w in range(2):
        at = 256 * (w + 1)
        acc = jnp.sum(wide[0:128] * wide[at:at + 128].T, axis=0, keepdims=True)
        acc = acc + jnp.sum(wide[128:256] * wide[at + 128:at + 256].T, axis=0, keepdims=True)
        sums.append(acc)
    sums.append(jnp.zeros((14, 128), F32))
    out[768:784] = jnp.concatenate(sums, axis=0).astype(BF16)


def own_points(parts):
    return pl.pallas_call(
        own_kernel,
        in_specs=[VM],
        out_specs=[VM, VM],
        out_shape=[jax.ShapeDtypeStruct((PAY, 128), BF16), jax.ShapeDtypeStruct((8, 256, 128), BF16)],
        compiler_params=LIMIT,
        cost_estimate=cost(1 << 24, 2 << 20),
        name="own",
    )(parts)


def make_exchange_kernel(shapes, which, first, last):
    def kernel(pos, *refs):
        count = len(shapes)
        held, (vals, same, cross), rest = refs[:count], refs[count:count + 3], refs[count + 3:]
        pays = []
        for ref, shape in zip(held, shapes):
            pays += [ref] if len(shape) == 2 else [ref.at[0], ref.at[1]]
        if first:
            e_out, u_out = rest
        elif last:
            e_in, u_in, f_low, f_high = rest
        else:
            e_in, u_in, e_out, u_out = rest
        flag = pos[0] == 0

        def theta(w):
            at = 256 * (w + 1)
            return jnp.concatenate(
                [jnp.concatenate([p[at:at + 128], p[at + 128:at + 256]], axis=1) for p in pays], axis=0
            )

        def chip_step(chip):
            xp = jnp.concatenate([p[0:256] for p in pays], axis=1)
            dens = jnp.concatenate([p[768:784] for p in pays], axis=1)
            lanes = pl.ds(pl.multiple_of(256 * chip, 256), 256)
            a = same[chip]
            b = cross[chip]
            xq = jnp.concatenate([jnp.where(flag, a, b), jnp.where(flag, b, a)], axis=1)
            v = jnp.concatenate([vals[n, :, lanes] for n in which], axis=0)
            u = dot(dens, v, ((1,), (0,)))
            if not first:
                u = u + u_in[:, lanes]
            if not last:
                u_out[:, lanes] = u
            wide = v.astype(F32)
            for w in range(2):
                tile = dot(theta(w), xq, ((1,), (0,)))
                amp = (wide * tile).astype(BF16)
                e = dot(xp, amp, ((1,), (0,)))
                rows = slice(256 * w, 256 * (w + 1))
                if not first:
                    e = e + e_in[rows, lanes]
                if not last:
                    e_out[rows, lanes] = e
                else:
                    f = (u[w:w + 1] * xq.astype(F32) - e).astype(BF16)
                    here = pl.ds(pl.multiple_of(128 * chip, 128), 128)
                    low, high = f[:, 0:128], f[:, 128:256]
                    f_low[rows, here] = jnp.where(flag, low, high)
                    f_high[rows, here] = jnp.where(flag, high, low)

        def pair_step(h, _):
            chip_step(2 * h)
            chip_step(2 * h + 1)
            return 0

        lax.fori_loop(0, 4, pair_step, 0)

    return kernel


def exchange(pos, held, which, vals, same, cross, totals, last=False):
    first = totals is None
    args = [pos, *held, vals, same, cross]
    alias = {}
    out_shape = [jax.ShapeDtypeStruct((512, 2048), F32), jax.ShapeDtypeStruct((16, 2048), F32)]
    if last:
        out_shape = [jax.ShapeDtypeStruct((512, 1024), BF16)] * 2
    if not first:
        if not last:
            alias = {len(args): 0, len(args) + 1: 1}
        args += list(totals)
    return pl.pallas_call(
        make_exchange_kernel([a.shape for a in held], which, first, last),
        in_specs=[SM] + [VM] * (len(args) - 1),
        out_specs=[VM, VM],
        out_shape=out_shape,
        input_output_aliases=alias,
        compiler_params=LIMIT,
        cost_estimate=cost(1024 * len(which) * 2048 * 256, 8 << 20),
        name="exchange",
    )(*args)


def decode_kernel(pos, f_mine, f_got, *refs):
    cols = refs[:8]
    keep, give = refs[8:]
    f = (f_mine[...].astype(F32) + f_got[...].astype(F32)).astype(BF16)
    for j in range(8):
        chip = lax.bitwise_xor(pos[17], j // 4) * 4 + lax.rem(pos[18] - j % 4 + 4, 4)
        g = dot(f, jnp.concatenate([cols[j][0], cols[j][1]], axis=1), ((1,), (0,)))
        keep[chip] = g[:, 0:128].astype(BF16)
        give[chip] = g[:, 128:256].astype(BF16)


def decode(pos, f, f_got, cols):
    return pl.pallas_call(
        decode_kernel,
        in_specs=[SM] + [VM] * 10,
        out_specs=[VM, VM],
        out_shape=[jax.ShapeDtypeStruct((8, 512, 128), BF16)] * 2,
        compiler_params=LIMIT,
        cost_estimate=cost(2 * 512 * 1024 * 2048, 8 << 20),
        name="decode",
    )(pos, f, f_got, *cols)


def sum_kernel(parts, out):
    total = parts[0].astype(F32)
    for j in range(1, 8):
        total = total + parts[j].astype(F32)
    total = total.astype(BF16)
    for w in range(2):
        for c in range(16):
            out[c, w] = total[256 * w + 16 * c:256 * w + 16 * (c + 1)]


def program(collocation, greens, trial_orbitals, coulomb):
    yl, x, c = lax.axis_index("yl"), lax.axis_index("x"), lax.axis_index("c")
    z, yh = lax.axis_index("z"), lax.axis_index("yh")

    def place(step, flip):
        return lax.rem(z - step + 8, 8) * 2 + (yh if flip == 0 else 1 - yh)

    order = [(0, 0), (0, 1)]
    for s in (1, 2, 3):
        order += [(s, 0), (s, 1), (-s, 0), (-s, 1)]
    order += [(4, 0), (-4, 1)]
    pos = jnp.stack([c] + [place(*k) for k in order] + [yl, x]).astype(jnp.int32)

    coulomb = pltpu.with_memory_space_constraint(coulomb, pltpu.HBM)
    halves = collocation.reshape(8, 2, 128, 128)
    mine = lax.dynamic_index_in_dim(halves, c, 1, keepdims=False)
    give = lax.dynamic_index_in_dim(halves, 1 - c, 1, keepdims=False)
    stacked = jnp.concatenate([trial_orbitals, greens.reshape(512, 128)], axis=0)
    got = lax.ppermute(give, "c", swap())
    other = lax.ppermute(stacked, "c", swap())
    partial_value = encode(mine, got, stacked, other)
    parts = lax.all_to_all(partial_value, CHIPS, 0, 0, tiled=True)
    own, spread = own_points(parts)

    mate = lax.ppermute(own, "yh", swap())
    pair = jnp.stack([own, mate])
    same = lax.all_to_all(spread, CHIPS, 0, 0, tiled=True)
    cross = lax.ppermute(same, "c", swap())
    up, down = [pair], [pair]
    for _ in range(3):
        up.append(lax.ppermute(up[-1], "z", ring(8, 1)))
        down.append(lax.ppermute(down[-1], "z", ring(8, -1)))
    last_up, last_down = up[3][0], down[3][1]
    far_up = lax.ppermute(last_up, "z", ring(8, 1))
    far_down = lax.ppermute(last_down, "z", ring(8, -1))
    far = [far_up, far_down]
    base = jnp.stack([mine.reshape(1024, 128), got.reshape(1024, 128)])
    base, _ = lax.optimization_barrier((base, pair))
    cols = [base] + [None] * 7
    cols[4] = lax.ppermute(base, "yl", swap())
    cols[1] = lax.ppermute(base, "x", ring(4, 1))
    cols[3] = lax.ppermute(base, "x", ring(4, -1))
    cols[2] = lax.ppermute(cols[1], "x", ring(4, 1))
    cols[7] = lax.ppermute(cols[4], "x", ring(4, -1))
    cols[5] = lax.ppermute(cols[4], "x", ring(4, 1))
    cols[6] = lax.ppermute(cols[2], "yl", swap())
    pos, _ = lax.optimization_barrier((pos, pair))
    rows = fetch(pos, coulomb)
    totals = exchange(pos, [pair, up[1], down[1]], NEAR, rows, same, cross, None)
    totals = exchange(pos, [up[2], down[2]], MIDDLE, rows, same, cross, totals)
    f_mine, f_give = exchange(pos, [up[3], down[3], *far], LAST, rows, same, cross, totals, True)
    f_got = lax.ppermute(f_give, "c", swap())
    keep, send = decode(pos, f_mine, f_got, cols)
    back = lax.ppermute(send, "c", swap())
    both = (keep.astype(F32) + back.astype(F32)).astype(BF16)
    terms = lax.all_to_all(both, CHIPS, 0, 0, tiled=True)
    summed = pl.pallas_call(
        sum_kernel,
        in_specs=[VM],
        out_specs=VM,
        out_shape=jax.ShapeDtypeStruct((16, 2, 16, 128), BF16),
        compiler_params=LIMIT,
        name="chip_sum",
    )(terms)
    shares = lax.all_to_all(summed.reshape(16, 32, 128), COL, 0, 0, tiled=True).reshape(16, 2, 16, 128)
    total = jnp.sum(shares.astype(F32), axis=0) * P_SIZE ** (-0.5)
    return jnp.swapaxes(total, 0, 1).astype(BF16)


def solution(mesh):
    finer = Mesh(mesh.devices.reshape(2, 4, 2, 8, 2), ("yl", "x", "c", "z", "yh"))
    placed = (P(COL, ROW), P(None, None, ROW), P(None, ROW), P(None, ROW, COL))
    return jax.shard_map(
        program, mesh=finer, in_specs=placed, out_specs=P(COL, None, ROW), check_vma=False
    )
```

```python
import jax
import jax.numpy as jnp
from jax import lax
from jax.experimental import pallas as pl
from jax.experimental.pallas import tpu as pltpu
from jax.sharding import Mesh
from jax.sharding import PartitionSpec as P

P_SIZE = 32768
ROW = ("yl", "x", "c")
CHIPS = ("yl", "x")
COL = ("z", "yh")
F32 = jnp.float32
BF16 = jnp.bfloat16
PAY = 784
NEAR, MIDDLE, OUTER, LAST = range(0, 6), range(6, 10), range(10, 14), range(14, 16)
LIMIT = pltpu.CompilerParams(vmem_limit_bytes=8 * 1024 * 1024)
VM = pl.BlockSpec(memory_space=pltpu.VMEM)
SM = pl.BlockSpec(memory_space=pltpu.SMEM)
HB = pl.BlockSpec(memory_space=pltpu.HBM)


def swap():
    return [(0, 1), (1, 0)]


def ring(size, step):
    return [(i, (i + step) % size) for i in range(size)]


def dot(a, b, dims):
    return lax.dot_general(a, b, (dims, ((), ())), preferred_element_type=F32)


def cost(flops, moved):
    return pl.CostEstimate(flops=flops, transcendentals=0, bytes_accessed=moved)


def encode_kernel(mine, got, stacked, other, out):
    def step(j, _):
        rows = jnp.concatenate([mine[j], got[j]], axis=1)
        x_side = jnp.concatenate([stacked[0:256], other[0:256]], axis=1)
        out[j, :, 0:128] = dot(x_side, rows, ((1,), (1,))).astype(BF16)
        for w in range(2):
            here = slice(256 * (w + 1), 256 * (w + 2))
            side = jnp.concatenate([stacked[here], other[here]], axis=1)
            theta = dot(rows, side, ((1,), (1,))).astype(BF16)
            for h in range(2):
                lanes = slice(128 * (w + 1), 128 * (w + 2))
                out[j, 128 * h:128 * (h + 1), lanes] = theta[:, 128 * h:128 * (h + 1)]
        return 0

    lax.fori_loop(0, 8, step, 0, unroll=2)


def encode(*args):
    return pl.pallas_call(
        encode_kernel,
        in_specs=[VM] * 4,
        out_specs=VM,
        out_shape=jax.ShapeDtypeStruct((8, 256, 384), BF16),
        compiler_params=LIMIT,
        cost_estimate=cost(2 * 1024 * 256 * 768, 3 << 20),
        name="encode",
    )(*args)


def fetch_kernel(pos, kern, rows, sems):
    copies = [pltpu.make_async_copy(kern.at[pos[1 + n]], rows.at[n], sems.at[n]) for n in range(16)]
    for copy in copies:
        copy.start()
    for copy in copies:
        copy.wait()


def fetch(pos, coulomb):
    return pl.pallas_call(
        fetch_kernel,
        in_specs=[SM, HB],
        out_specs=VM,
        out_shape=jax.ShapeDtypeStruct((16, 128, 2048), BF16),
        scratch_shapes=[pltpu.SemaphoreType.DMA((16,))],
        compiler_params=LIMIT,
        cost_estimate=cost(1 << 20, 8 << 20),
        name="fetch",
    )(pos, coulomb)


def own_kernel(parts, out, spread):
    total = parts[0].astype(F32)
    for j in range(1, 8):
        total = total + parts[j].astype(F32)
    total = jnp.concatenate([total[:, 128 * n:128 * (n + 1)] for n in range(3)], axis=0).astype(BF16)
    out[0:768] = total
    for j in range(8):
        spread[j] = total[0:256]
    wide = total.astype(F32)
    sums = []
    for w in range(2):
        at = 256 * (w + 1)
        acc = jnp.sum(wide[0:128] * wide[at:at + 128].T, axis=0, keepdims=True)
        acc = acc + jnp.sum(wide[128:256] * wide[at + 128:at + 256].T, axis=0, keepdims=True)
        sums.append(acc)
    sums.append(jnp.zeros((14, 128), F32))
    out[768:784] = jnp.concatenate(sums, axis=0).astype(BF16)


def own_points(parts):
    return pl.pallas_call(
        own_kernel,
        in_specs=[VM],
        out_specs=[VM, VM],
        out_shape=[jax.ShapeDtypeStruct((PAY, 128), BF16), jax.ShapeDtypeStruct((8, 256, 128), BF16)],
        compiler_params=LIMIT,
        cost_estimate=cost(1 << 24, 2 << 20),
        name="own",
    )(parts)


def make_exchange_kernel(shapes, which, first, last):
    def kernel(pos, *refs):
        count = len(shapes)
        held, (vals, same, cross), rest = refs[:count], refs[count:count + 3], refs[count + 3:]
        pays = []
        for ref, shape in zip(held, shapes):
            pays += [ref] if len(shape) == 2 else [ref.at[0], ref.at[1]]
        if first:
            e_out, u_out = rest
        elif last:
            e_in, u_in, f_low, f_high = rest
        else:
            e_in, u_in, e_out, u_out = rest
        flag = pos[0] == 0

        def theta(w):
            at = 256 * (w + 1)
            return jnp.concatenate(
                [jnp.concatenate([p[at:at + 128], p[at + 128:at + 256]], axis=1) for p in pays], axis=0
            )

        def chip_step(chip):
            xp = jnp.concatenate([p[0:256] for p in pays], axis=1)
            dens = jnp.concatenate([p[768:784] for p in pays], axis=1)
            lanes = pl.ds(pl.multiple_of(256 * chip, 256), 256)
            a = same[chip]
            b = cross[chip]
            xq = jnp.concatenate([jnp.where(flag, a, b), jnp.where(flag, b, a)], axis=1)
            v = jnp.concatenate([vals[n, :, lanes] for n in which], axis=0)
            u = dot(dens, v, ((1,), (0,)))
            if not first:
                u = u + u_in[:, lanes]
            if not last:
                u_out[:, lanes] = u
            wide = v.astype(F32)
            for w in range(2):
                tile = dot(theta(w), xq, ((1,), (0,)))
                amp = (wide * tile).astype(BF16)
                e = dot(xp, amp, ((1,), (0,)))
                rows = slice(256 * w, 256 * (w + 1))
                if not first:
                    e = e + e_in[rows, lanes]
                if not last:
                    e_out[rows, lanes] = e
                else:
                    f = (u[w:w + 1] * xq.astype(F32) - e).astype(BF16)
                    here = pl.ds(pl.multiple_of(128 * chip, 128), 128)
                    low, high = f[:, 0:128], f[:, 128:256]
                    f_low[rows, here] = jnp.where(flag, low, high)
                    f_high[rows, here] = jnp.where(flag, high, low)

        def pair_step(h, _):
            chip_step(2 * h)
            chip_step(2 * h + 1)
            return 0

        lax.fori_loop(0, 4, pair_step, 0)

    return kernel


def exchange(pos, held, which, vals, same, cross, totals, last=False):
    first = totals is None
    args = [pos, *held, vals, same, cross]
    alias = {}
    out_shape = [jax.ShapeDtypeStruct((512, 2048), F32), jax.ShapeDtypeStruct((16, 2048), F32)]
    if last:
        out_shape = [jax.ShapeDtypeStruct((512, 1024), BF16)] * 2
    if not first:
        if not last:
            alias = {len(args): 0, len(args) + 1: 1}
        args += list(totals)
    return pl.pallas_call(
        make_exchange_kernel([a.shape for a in held], which, first, last),
        in_specs=[SM] + [VM] * (len(args) - 1),
        out_specs=[VM, VM],
        out_shape=out_shape,
        input_output_aliases=alias,
        compiler_params=LIMIT,
        cost_estimate=cost(1024 * len(which) * 2048 * 256, 8 << 20),
        name="exchange",
    )(*args)


def decode_kernel(pos, f_mine, f_got, *refs):
    cols = refs[:8]
    keep, give = refs[8:]
    f = (f_mine[...].astype(F32) + f_got[...].astype(F32)).astype(BF16)
    for j in range(8):
        chip = lax.bitwise_xor(pos[17], j // 4) * 4 + lax.rem(pos[18] - j % 4 + 4, 4)
        g = dot(f, jnp.concatenate([cols[j][0], cols[j][1]], axis=1), ((1,), (0,)))
        keep[chip] = g[:, 0:128].astype(BF16)
        give[chip] = g[:, 128:256].astype(BF16)


def decode(pos, f, f_got, cols):
    return pl.pallas_call(
        decode_kernel,
        in_specs=[SM] + [VM] * 10,
        out_specs=[VM, VM],
        out_shape=[jax.ShapeDtypeStruct((8, 512, 128), BF16)] * 2,
        compiler_params=LIMIT,
        cost_estimate=cost(2 * 512 * 1024 * 2048, 8 << 20),
        name="decode",
    )(pos, f, f_got, *cols)


def sum_kernel(parts, out):
    total = parts[0].astype(F32)
    for j in range(1, 8):
        total = total + parts[j].astype(F32)
    total = total.astype(BF16)
    for w in range(2):
        for c in range(16):
            out[c, w] = total[256 * w + 16 * c:256 * w + 16 * (c + 1)]


def program(collocation, greens, trial_orbitals, coulomb):
    yl, x, c = lax.axis_index("yl"), lax.axis_index("x"), lax.axis_index("c")
    z, yh = lax.axis_index("z"), lax.axis_index("yh")

    def place(step, flip):
        return lax.rem(z - step + 8, 8) * 2 + (yh if flip == 0 else 1 - yh)

    order = [(0, 0), (0, 1)]
    for s in (1, 2, 3):
        order += [(s, 0), (s, 1), (-s, 0), (-s, 1)]
    order += [(4, 0), (-4, 1)]
    pos = jnp.stack([c] + [place(*k) for k in order] + [yl, x]).astype(jnp.int32)

    coulomb = pltpu.with_memory_space_constraint(coulomb, pltpu.HBM)
    halves = collocation.reshape(8, 2, 128, 128)
    mine = lax.dynamic_index_in_dim(halves, c, 1, keepdims=False)
    give = lax.dynamic_index_in_dim(halves, 1 - c, 1, keepdims=False)
    stacked = jnp.concatenate([trial_orbitals, greens.reshape(512, 128)], axis=0)
    got = lax.ppermute(give, "c", swap())
    other = lax.ppermute(stacked, "c", swap())
    partial_value = encode(mine, got, stacked, other)
    parts = lax.all_to_all(partial_value, CHIPS, 0, 0, tiled=True)
    own, spread = own_points(parts)

    mate = lax.ppermute(own, "yh", swap())
    pair = jnp.stack([own, mate])
    same = lax.all_to_all(spread, CHIPS, 0, 0, tiled=True)
    cross = lax.ppermute(same, "c", swap())
    up, down = [pair], [pair]
    for _ in range(3):
        up.append(lax.ppermute(up[-1], "z", ring(8, 1)))
        down.append(lax.ppermute(down[-1], "z", ring(8, -1)))
    last_up, last_down = up[3][0], down[3][1]
    far_up = lax.ppermute(last_up, "z", ring(8, 1))
    far_down = lax.ppermute(last_down, "z", ring(8, -1))
    far = [far_up, far_down]
    base = jnp.stack([mine.reshape(1024, 128), got.reshape(1024, 128)])
    base, _ = lax.optimization_barrier((base, pair))
    cols = [base] + [None] * 7
    cols[4] = lax.ppermute(base, "yl", swap())
    cols[1] = lax.ppermute(base, "x", ring(4, 1))
    cols[3] = lax.ppermute(base, "x", ring(4, -1))
    cols[2] = lax.ppermute(cols[1], "x", ring(4, 1))
    cols[7] = lax.ppermute(cols[4], "x", ring(4, -1))
    cols[5] = lax.ppermute(cols[4], "x", ring(4, 1))
    cols[6] = lax.ppermute(cols[2], "yl", swap())
    pos, _ = lax.optimization_barrier((pos, pair))
    rows = fetch(pos, coulomb)
    totals = exchange(pos, [pair, up[1], down[1]], NEAR, rows, same, cross, None)
    totals = exchange(pos, [up[2], down[2]], MIDDLE, rows, same, cross, totals)
    totals = exchange(pos, [up[3], down[3]], OUTER, rows, same, cross, totals)
    f_mine, f_give = exchange(pos, far, LAST, rows, same, cross, totals, True)
    f_got = lax.ppermute(f_give, "c", swap())
    keep, send = decode(pos, f_mine, f_got, cols)
    back = lax.ppermute(send, "c", swap())
    both = (keep.astype(F32) + back.astype(F32)).astype(BF16)
    terms = lax.all_to_all(both, CHIPS, 0, 0, tiled=True)
    summed = pl.pallas_call(
        sum_kernel,
        in_specs=[VM],
        out_specs=VM,
        out_shape=jax.ShapeDtypeStruct((16, 2, 16, 128), BF16),
        compiler_params=LIMIT,
        name="chip_sum",
    )(terms)
    shares = lax.all_to_all(summed.reshape(16, 32, 128), COL, 0, 0, tiled=True).reshape(16, 2, 16, 128)
    total = jnp.sum(shares.astype(F32), axis=0) * P_SIZE ** (-0.5)
    return jnp.swapaxes(total, 0, 1).astype(BF16)


def solution(mesh):
    finer = Mesh(mesh.devices.reshape(2, 4, 2, 8, 2), ("yl", "x", "c", "z", "yh"))
    placed = (P(COL, ROW), P(None, None, ROW), P(None, ROW), P(None, ROW, COL))
    return jax.shard_map(
        program, mesh=finer, in_specs=placed, out_specs=P(COL, None, ROW), check_vma=False
    )
```
